512 devices in a mesh: expert: 128 (over x, z, y_lo), hidden: 4 (over y_hi, core).
Axes of the slice: x: 4, y: 8 (y_hi: 2, y_lo: 4; y = y_hi * 4 + y_lo), z: 8, core: 2. Of those that a mesh axis runs over, the one named last changes fastest.
Arguments:
- tokens: bfloat16 [512, 196, 1024], P(('expert', 'hidden')), may hold values from -40 to 40
- router: bfloat16 [1024, 128], replicated, may hold values from -0.5 to 0.5
- w_in: bfloat16 [128, 1024, 3072], P('expert', None, 'hidden'), may hold values from -0.1875 to 0.1875
- b_in: float32 [128, 3072], P('expert', 'hidden'), may hold values from -6 to 6
- w_out: bfloat16 [128, 3072, 1024], P('expert', 'hidden'), may hold values from -0.109375 to 0.109375
- cotangent: bfloat16 [512, 196, 1024], P(('expert', 'hidden')), may hold values from -6 to 6
Outputs:
- mixed: bfloat16 [512, 196, 1024], P(('expert', 'hidden'))
- token_grad: bfloat16 [512, 196, 1024], P(('expert', 'hidden'))
The draws below stay inside these ranges and needn't reach their ends.
All inputs are finite; a program needn't handle non-finite values.
Results may differ from the reference program's by a relative error of at most 0.015.
Values may be sent and summed in bfloat16 or wider, within the bound.
No kernel may reach another device: no remote copies, remote signals or barrier semaphores. Data moves between devices by JAX's collectives and lax.ppermute only.
A program may use at most 64 MiB of HBM per device.

```python
import math
import jax
import jax.numpy as jnp
from jax import lax

D = 1024
FF = 3072
M = 196
EXPERTS = 128
IMAGES = 512
N_HIDDEN = 4


def build_router(key):
    inner = jax.random.fold_in(key, 11)
    raw = jax.random.normal(inner, (D, EXPERTS), jnp.float32) * (2.0 / math.sqrt(D))
    return jnp.clip(raw, -0.5, 0.5).astype(jnp.bfloat16).astype(jnp.float32)


def draw_router(key, part):
    return build_router(key).astype(jnp.bfloat16)


def draw_tokens(key, part):
    inner = jax.random.fold_in(key, 23)
    base = jnp.clip(jax.random.normal(inner, (IMAGES, M, D), jnp.float32), -6.0, 6.0)
    return jnp.clip(base, -40.0, 40.0).astype(jnp.bfloat16)


def block_levels(key, dims, cuts, least, largest):
    level = 1.0
    for dim, blocks in cuts:
        heights = jax.random.uniform(jax.random.fold_in(jax.random.fold_in(key, 6), dim), (blocks,), jnp.float32, least / len(cuts), largest / len(cuts))
        level = level * jnp.repeat(jnp.exp(heights), dims[dim] // blocks).reshape((-1,) + (1,) * (len(dims) - 1 - dim))
    return level


def scatter_about(rng, extent, width, most, cuts=(), held_as=jnp.bfloat16):
    values = width * jax.random.normal(rng, extent, jnp.float32)
    if cuts:
        values = values * block_levels(rng, extent, cuts, -0.22, 0.18)
    return jnp.clip(values, -most, most).astype(held_as)


def setup_inputs(seed: int = 0) -> dict:
    arg_keys = jax.random.split(jax.random.key(seed), 7)
    return {
        "tokens": draw_tokens(jax.random.fold_in(arg_keys[6], 71), 0),
        "router": draw_router(jax.random.fold_in(arg_keys[6], 71), 0),
        "w_in": scatter_about(arg_keys[2], (EXPERTS, D, FF), D ** -0.5, 0.1875, ((0, 128), (2, 4))),
        "b_in": scatter_about(arg_keys[3], (EXPERTS, FF), 1.0, 6.0, ((0, 128), (1, 4)), jnp.float32),
        "w_out": scatter_about(arg_keys[4], (EXPERTS, FF, D), FF ** -0.5, 0.109375, ((0, 128), (1, 4))),
        "cotangent": scatter_about(arg_keys[5], (IMAGES, M, D), 1.0, 6.0, ((0, 512),)),
    }


def expert_rows(packed):
    rows, grads, weight_in, bias_in, weight_out = packed
    count = rows.shape[0]
    quarter = FF // N_HIDDEN
    pre = jnp.dot(rows, weight_in, preferred_element_type=jnp.float32) + bias_in
    act = jax.nn.gelu(pre).astype(jnp.bfloat16)
    parts = jnp.einsum('bhf,hfd->hbd', act.reshape(count, N_HIDDEN, quarter).astype(jnp.float32), weight_out.reshape(N_HIDDEN, quarter, D).astype(jnp.float32)).astype(jnp.bfloat16)
    slot_out = lax.optimization_barrier(jnp.sum(parts.astype(jnp.float32), axis=0)).astype(jnp.bfloat16)
    act_grad = jnp.dot(grads, weight_out.T, preferred_element_type=jnp.float32)
    _, pull = jax.vjp(jax.nn.gelu, pre)
    pre_grad = pull(act_grad)[0].astype(jnp.bfloat16)
    gparts = jnp.einsum('bhf,dhf->hbd', pre_grad.reshape(count, N_HIDDEN, quarter).astype(jnp.float32), weight_in.reshape(D, N_HIDDEN, quarter).astype(jnp.float32)).astype(jnp.bfloat16)
    slot_grad = lax.optimization_barrier(jnp.sum(gparts.astype(jnp.float32), axis=0)).astype(jnp.bfloat16)
    return (slot_out, slot_grad)

def reference(tokens, router, w_in, b_in, w_out, cotangent):
    tok32 = tokens.astype(jnp.float32)
    cot32 = cotangent.astype(jnp.float32)
    router32 = router.astype(jnp.float32)
    logits = jnp.einsum('bmd,ds->bms', tok32, router32)
    dispatch = jax.nn.softmax(logits, axis=1)
    combine = jax.nn.softmax(logits, axis=2)
    dispatch_w = dispatch.astype(jnp.bfloat16)
    combine_w = combine.astype(jnp.bfloat16)
    slot_in = jnp.einsum('bms,bmd->bsd', dispatch_w.astype(jnp.float32), tok32).astype(jnp.bfloat16)
    slot_cot = jnp.einsum('bms,bmd->bsd', combine_w.astype(jnp.float32), cot32).astype(jnp.bfloat16)
    slot_out, slot_grad = lax.map(expert_rows, (jnp.transpose(slot_in, (1, 0, 2)), jnp.transpose(slot_cot, (1, 0, 2)), w_in, b_in, w_out))
    slot_out = jnp.transpose(slot_out, (1, 0, 2)).astype(jnp.float32)
    slot_grad = jnp.transpose(slot_grad, (1, 0, 2)).astype(jnp.float32)
    mixed = jnp.einsum('bms,bsd->bmd', combine_w.astype(jnp.float32), slot_out).astype(jnp.bfloat16)
    combine_grad = jnp.einsum('bmd,bsd->bms', cot32, slot_out)
    dispatch_grad = jnp.einsum('bmd,bsd->bms', tok32, slot_grad)
    logit_grad = combine * (combine_grad - lax.optimization_barrier(jnp.sum(combine * combine_grad, axis=2, keepdims=True)))
    logit_grad = logit_grad + dispatch * (dispatch_grad - lax.optimization_barrier(jnp.sum(dispatch * dispatch_grad, axis=1, keepdims=True)))
    logit_grad = logit_grad.astype(jnp.bfloat16)
    token_grad = jnp.einsum('bms,bsd->bmd', dispatch_w.astype(jnp.float32), slot_grad)
    token_grad = token_grad + jnp.einsum('bms,ds->bmd', logit_grad.astype(jnp.float32), router32)
    return (mixed, token_grad.astype(jnp.bfloat16))
```

```python
import jax
import jax.numpy as jnp
from jax import lax
from jax.sharding import Mesh, PartitionSpec as P

CHIPS = ("expert", "yh")
SPLIT = False


def swap_cores(x):
    return lax.ppermute(x, "core", [(0, 1), (1, 0)])


def exchange(x):
    return lax.all_to_all(x, CHIPS, 0, 0, tiled=True)


def experts(rows, grads, halves):
    value = 0.0
    gvalue = 0.0
    for w_in, b_in, w_out in halves:
        pre = jnp.einsum("rd,df->rf", rows, w_in, preferred_element_type=jnp.float32) + b_in
        act, pull = jax.vjp(jax.nn.gelu, pre)
        value = value + jnp.einsum(
            "rf,fd->rd", act.astype(jnp.bfloat16), w_out, preferred_element_type=jnp.float32
        )
        act_grad = jnp.einsum("rd,fd->rf", grads, w_out, preferred_element_type=jnp.float32)
        pre_grad = pull(act_grad)[0].astype(jnp.bfloat16)
        gvalue = gvalue + jnp.einsum(
            "rf,df->rd", pre_grad, w_in, preferred_element_type=jnp.float32
        )
    return value.astype(jnp.bfloat16), gvalue.astype(jnp.bfloat16)


def shards(tokens, router, w_in, b_in, w_out, cotangent):
    tokens, w_in, w_out, cotangent = tokens[0], w_in[0], w_out[0], cotangent[0]
    own = (w_in, b_in, w_out)
    other = tuple(swap_cores(w) for w in own)
    logits = jnp.einsum("md,ds->ms", tokens, router, preferred_element_type=jnp.float32)
    dispatch = jax.nn.softmax(logits, axis=0)
    combine = jax.nn.softmax(logits, axis=1)
    dispatch_w = dispatch.astype(jnp.bfloat16)
    combine_w = combine.astype(jnp.bfloat16)
    slot_in = jnp.einsum(
        "ms,md->sd", dispatch_w, tokens, preferred_element_type=jnp.float32
    ).astype(jnp.bfloat16)
    slot_cot = jnp.einsum(
        "ms,md->sd", combine_w, cotangent, preferred_element_type=jnp.float32
    ).astype(jnp.bfloat16)
    slots, width = slot_in.shape
    ways = lax.axis_size("yh")
    both = jnp.stack([slot_in, slot_cot], axis=1)
    both = jnp.broadcast_to(both[:, None], (slots, ways, 2, width)).reshape(slots * ways, 2, width)
    arrived = exchange(both)
    value, gvalue = experts(arrived[:, 0], arrived[:, 1], (own, other))
    returned = exchange(jnp.stack([value, gvalue], axis=1)).astype(jnp.float32)
    summed = returned.reshape(slots, ways, 2, width).sum(axis=1).astype(jnp.bfloat16)
    slot_out = summed[:, 0]
    slot_grad = summed[:, 1]
    mixed = jnp.einsum(
        "ms,sd->md", combine_w, slot_out, preferred_element_type=jnp.float32
    ).astype(jnp.bfloat16)
    combine_grad = jnp.einsum(
        "md,sd->ms", cotangent, slot_out, preferred_element_type=jnp.float32
    )
    dispatch_grad = jnp.einsum(
        "md,sd->ms", tokens, slot_grad, preferred_element_type=jnp.float32
    )
    logit_grad = combine * (combine_grad - jnp.sum(combine * combine_grad, axis=1, keepdims=True))
    logit_grad = logit_grad + dispatch * (
        dispatch_grad - jnp.sum(dispatch * dispatch_grad, axis=0, keepdims=True)
    )
    logit_grad = logit_grad.astype(jnp.bfloat16)
    token_grad = jnp.einsum(
        "ms,sd->md", dispatch_w, slot_grad, preferred_element_type=jnp.float32
    )
    token_grad = token_grad + jnp.einsum(
        "ms,ds->md", logit_grad, router, preferred_element_type=jnp.float32
    )
    return mixed[None], token_grad.astype(jnp.bfloat16)[None]


def solution(mesh):
    ways = mesh.shape["hidden"] // 2
    split = Mesh(
        mesh.devices.reshape(mesh.shape["expert"], ways, 2), ("expert", "yh", "core")
    )
    images = P(("expert", "yh", "core"), None, None)
    hidden = ("yh", "core")
    return jax.shard_map(
        shards,
        mesh=split,
        in_specs=(
            images,
            P(),
            P("expert", None, hidden),
            P("expert", hidden),
            P("expert", hidden, None),
            images,
        ),
        out_specs=(images, images),
        check_vma=False,
    )
```

```python
import jax
import jax.numpy as jnp
from jax import lax
from jax.experimental import pallas as pl
from jax.experimental.pallas import tpu as pltpu
from jax.sharding import Mesh, PartitionSpec as P

CHIPS = ("expert", "yh")
LANES = 128
UNITS = 256
BLOCKS = 4
PIECES = 1
NN = (((1,), (0,)), ((), ()))
NT = (((1,), (1,)), ((), ()))
TN = (((0,), (0,)), ((), ()))
GELU_A = 0.7978845608028654
GELU_B = 0.044715


def in_hbm(*arrays):
    return [pltpu.with_memory_space_constraint(x, pltpu.HBM) for x in arrays]


def dot(a, b, dims):
    return lax.dot_general(a, b, dims, preferred_element_type=jnp.float32)


def spread(scratch, values, first, step, column):
    rows = values.shape[0]
    for k in range(values.shape[1] // LANES):
        piece = values[:, k * LANES : (k + 1) * LANES]
        scratch[pl.ds(first + column // LANES + k, rows, stride=step), :] = piece


def gather(scratch, out, rows, first, step):
    for k in range(out.shape[1] // LANES):
        piece = scratch[pl.ds(first + k, rows, stride=step), :]
        out[:, k * LANES : (k + 1) * LANES] = piece.astype(out.dtype)


def route_kernel(
    tokens, router, cotangent, sent, dispatch, combine, image, weights, pull, scratch, packed, sems
):
    width = image.shape[2]
    slots = weights.shape[1]
    tiles = 2 * width // LANES
    ways = sent.shape[1] // tiles
    loads = [
        pltpu.make_async_copy(src, dst, sems.at[k])
        for k, (src, dst) in enumerate(((tokens, image), (router, weights), (cotangent, pull)))
    ]
    for load in loads:
        load.start()
    loads[0].wait()
    loads[1].wait()
    logits = dot(image[0], weights[...], NN)
    up = jnp.exp(logits - jnp.max(logits, axis=0, keepdims=True))
    down = up / jnp.sum(up, axis=0, keepdims=True)
    dispatch[...] = down
    down = down.astype(jnp.bfloat16)
    up = jnp.exp(logits - jnp.max(logits, axis=1, keepdims=True))
    across = up / jnp.sum(up, axis=1, keepdims=True)
    combine[...] = across
    across = across.astype(jnp.bfloat16)
    for n in range(0, width, 256):
        spread(scratch, dot(down, image[0, :, n : n + 256], TN), 0, tiles, n)
    loads[2].wait()
    for n in range(0, width, 256):
        spread(scratch, dot(across, pull[0, :, n : n + 256], TN), tiles // 2, tiles, n)
    stores = []
    block = slots // BLOCKS
    for k in range(BLOCKS):
        part = pl.ds(k * block, block)
        piece = scratch[pl.ds(k * block * tiles, block * tiles), :].astype(jnp.bfloat16)
        piece = piece.reshape(block, tiles, LANES)
        for way in range(ways):
            packed[part, way * tiles : (way + 1) * tiles, :] = piece
        stores.append(pltpu.make_async_copy(packed.at[part], sent.at[part], sems.at[3 + k]))
        stores[-1].start()
    for store in stores:
        store.wait()


def route(tokens, router, cotangent, ways):
    _, count, width = tokens.shape
    slots = router.shape[1]
    tiles = 2 * width // LANES
    weights = jax.ShapeDtypeStruct((count, slots), jnp.float32)
    return pl.pallas_call(
        route_kernel,
        out_shape=(
            pltpu.HBM((slots, ways * tiles, LANES), jnp.bfloat16),
            weights,
            weights,
        ),
        in_specs=[pl.BlockSpec(memory_space=pltpu.HBM)] * 3,
        out_specs=(
            pl.BlockSpec(memory_space=pltpu.HBM),
            pl.BlockSpec(memory_space=pltpu.VMEM),
            pl.BlockSpec(memory_space=pltpu.VMEM),
        ),
        scratch_shapes=[
            pltpu.VMEM(tokens.shape, jnp.bfloat16),
            pltpu.VMEM(router.shape, jnp.bfloat16),
            pltpu.VMEM(tokens.shape, jnp.bfloat16),
            pltpu.VMEM((slots * tiles, LANES), jnp.float32),
            pltpu.VMEM((slots, ways * tiles, LANES), jnp.bfloat16),
            pltpu.SemaphoreType.DMA((3 + BLOCKS,)),
        ],
        compiler_params=pltpu.CompilerParams(vmem_limit_bytes=16 * 2**20),
        name="route",
    )(*in_hbm(tokens, router, cotangent))


def expert_kernel(
    arrived, in0, b0, out0, in1, b1, out1, sent, near, first, far, scratch, rows, grads, act, slope, sems
):
    count, tiles, _ = arrived.shape
    half = tiles // 2
    width = half * LANES
    units = b0.shape[1]
    loads = []
    for k, (src, dst) in enumerate(((out0, near), (in1, first), (out1, far))):
        block = dst.shape[0] // PIECES
        loads.append([])
        for p in range(PIECES):
            part = pl.ds(p * block, block)
            copy = pltpu.make_async_copy(src.at[0, part], dst.at[part], sems.at[k, p])
            loads[k].append(copy)
            copy.start()
    scratch[...] = arrived[...].astype(jnp.float32).reshape(count * tiles, LANES)
    gather(scratch, rows, count, 0, tiles)
    gather(scratch, grads, count, half, tiles)
    for h, (w_in, bias, w_out) in enumerate(((in0.at[0], b0, near), (first, b1, far))):
        if h:
            for load in loads[1]:
                load.wait()
        for u in range(0, units, UNITS):
            part = slice(u, u + UNITS)
            at = slice(h * units + u, h * units + u + UNITS)
            pre = dot(rows[...], w_in[:, part], NN) + bias[:, part]
            if u == 0:
                for load in loads[2 * h]:
                    load.wait()
            up = dot(grads[...], w_out[part, :], NT)
            square = pre * pre
            tanh = jnp.tanh(GELU_A * (pre + GELU_B * (square * pre)))
            cdf = 0.5 + 0.5 * tanh
            bend = 0.5 * GELU_A * pre * (1.0 - tanh * tanh) * (1.0 + 3.0 * GELU_B * square)
            act[:, at] = (pre * cdf).astype(jnp.bfloat16)
            slope[:, at] = (up * (cdf + bend)).astype(jnp.bfloat16)
    for n in range(0, width, 256):
        part = slice(n, n + 256)
        value = dot(act[:, :units], near[:, part], NN) + dot(act[:, units:], far[:, part], NN)
        spread(scratch, value, 0, tiles, n)
        value = dot(slope[:, :units], in0[0, part, :], NT) + dot(slope[:, units:], first[part, :], NT)
        spread(scratch, value, half, tiles, n)
    sent[...] = scratch[...].astype(jnp.bfloat16).reshape(count, tiles, LANES)


def experts(arrived, own, other):
    count, tiles, _ = arrived.shape
    width = tiles // 2 * LANES
    units = own[1].shape[1]
    out0, in1, out1 = in_hbm(own[2], other[0], other[2])
    weight = pl.BlockSpec(memory_space=pltpu.HBM)
    local = pl.BlockSpec(memory_space=pltpu.VMEM)
    return pl.pallas_call(
        expert_kernel,
        out_shape=jax.ShapeDtypeStruct(arrived.shape, jnp.bfloat16),
        in_specs=[local, local, local, weight, weight, local, weight],
        out_specs=local,
        scratch_shapes=[
            pltpu.VMEM((units, width), jnp.bfloat16),
            pltpu.VMEM((width, units), jnp.bfloat16),
            pltpu.VMEM((units, width), jnp.bfloat16),
            pltpu.VMEM((count * tiles, LANES), jnp.float32),
            pltpu.VMEM((count, width), jnp.bfloat16),
            pltpu.VMEM((count, width), jnp.bfloat16),
            pltpu.VMEM((count, 2 * units), jnp.bfloat16),
            pltpu.VMEM((count, 2 * units), jnp.bfloat16),
            pltpu.SemaphoreType.DMA((3, PIECES)),
        ],
        compiler_params=pltpu.CompilerParams(vmem_limit_bytes=28 * 2**20),
        name="experts",
    )(arrived, own[0], own[1], out0, in1, other[1], out1)


def finish_kernel(
    returned,
    tokens,
    router,
    cotangent,
    dispatch,
    combine,
    mixed,
    token_grad,
    scratch,
    value,
    grad,
    near,
    far,
    sems,
):
    slots, width = value.shape
    tiles = 2 * width // LANES
    total = returned[:, :tiles, :].astype(jnp.float32)
    for way in range(1, returned.shape[1] // tiles):
        total = total + returned[:, way * tiles : (way + 1) * tiles, :].astype(jnp.float32)
    scratch[...] = total.reshape(slots * tiles, LANES)
    gather(scratch, value, slots, 0, tiles)
    gather(scratch, grad, slots, tiles // 2, tiles)
    down = dispatch[...]
    across = combine[...]
    near[0] = dot(across.astype(jnp.bfloat16), value[...], NN).astype(jnp.bfloat16)
    stores = [pltpu.make_async_copy(near, mixed, sems.at[0])]
    stores[0].start()
    pull = dot(cotangent[0], value[...], NT)
    slope = across * (pull - jnp.sum(across * pull, axis=1, keepdims=True))
    pull = dot(tokens[0], grad[...], NT)
    slope = slope + down * (pull - jnp.sum(down * pull, axis=0, keepdims=True))
    slope = slope.astype(jnp.bfloat16)
    down = down.astype(jnp.bfloat16)
    block = width // BLOCKS
    for k in range(BLOCKS):
        part = pl.ds(k * block, block)
        total = dot(down, grad[:, part], NN) + dot(slope, router[part, :], NT)
        far[0, :, part] = total.astype(jnp.bfloat16)
        stores.append(
            pltpu.make_async_copy(
                far.at[:, :, part], token_grad.at[:, :, part], sems.at[1 + k]
            )
        )
        stores[-1].start()
    for store in stores:
        store.wait()


def finish(returned, tokens, router, cotangent, dispatch, combine):
    width, slots = router.shape
    result = jax.ShapeDtypeStruct(tokens.shape, jnp.bfloat16)
    far = pl.BlockSpec(memory_space=pltpu.HBM)
    local = pl.BlockSpec(memory_space=pltpu.VMEM)
    return pl.pallas_call(
        finish_kernel,
        out_shape=(result, result),
        in_specs=[local] * 6,
        out_specs=(far, far),
        scratch_shapes=[
            pltpu.VMEM((slots * 2 * width // LANES, LANES), jnp.float32),
            pltpu.VMEM((slots, width), jnp.bfloat16),
            pltpu.VMEM((slots, width), jnp.bfloat16),
            pltpu.VMEM(tokens.shape, jnp.bfloat16),
            pltpu.VMEM(tokens.shape, jnp.bfloat16),
            pltpu.SemaphoreType.DMA((1 + BLOCKS,)),
        ],
        compiler_params=pltpu.CompilerParams(vmem_limit_bytes=16 * 2**20),
        name="finish",
    )(returned, tokens, router, cotangent, dispatch, combine)


def swap_cores(x):
    return lax.ppermute(x, "core", [(0, 1), (1, 0)])


def exchange(x):
    return lax.all_to_all(x, CHIPS, 0, 0, tiled=True)


def shards(tokens, router, w_in, b_in, w_out, cotangent):
    slots = router.shape[1]
    ways = lax.axis_size("yh")
    own = (w_in, b_in, w_out)
    other = tuple(swap_cores(w) for w in own)
    sent, dispatch, combine = route(tokens, router, cotangent, ways)
    tiles = sent.shape[1] // ways
    arrived = exchange(sent.reshape(slots * ways, tiles, LANES))
    returned = exchange(experts(arrived, own, other))
    returned = returned.reshape(slots, ways * tiles, LANES)
    return finish(returned, tokens, router, cotangent, dispatch, combine)


def solution(mesh):
    ways = mesh.shape["hidden"] // 2
    split = Mesh(
        mesh.devices.reshape(mesh.shape["expert"], ways, 2), ("expert", "yh", "core")
    )
    images = P(("expert", "yh", "core"), None, None)
    hidden = ("yh", "core")
    return jax.shard_map(
        shards,
        mesh=split,
        in_specs=(
            images,
            P(),
            P("expert", None, hidden),
            P("expert", hidden),
            P("expert", hidden, None),
            images,
        ),
        out_specs=(images, images),
        check_vma=False,
    )
```

```python
import jax
import jax.numpy as jnp
from jax import lax
from jax.experimental import pallas as pl
from jax.experimental.pallas import tpu as pltpu
from jax.sharding import Mesh, PartitionSpec as P

CHIPS = ("expert", "yh")
LANES = 128
UNITS = 256
BLOCKS = 4
STAGGER_NS = 11000
NN = (((1,), (0,)), ((), ()))
NT = (((1,), (1,)), ((), ()))
TN = (((0,), (0,)), ((), ()))
GELU_A = 0.7978845608028654
GELU_B = 0.044715


def in_hbm(*arrays):
    return [pltpu.with_memory_space_constraint(x, pltpu.HBM) for x in arrays]


def dot(a, b, dims):
    return lax.dot_general(a, b, dims, preferred_element_type=jnp.float32)


def spread(scratch, values, first, step, column):
    rows = values.shape[0]
    for k in range(values.shape[1] // LANES):
        piece = values[:, k * LANES : (k + 1) * LANES]
        scratch[pl.ds(first + column // LANES + k, rows, stride=step), :] = piece


def gather(scratch, out, rows, first, step):
    for k in range(out.shape[1] // LANES):
        piece = scratch[pl.ds(first + k, rows, stride=step), :]
        out[:, k * LANES : (k + 1) * LANES] = piece.astype(out.dtype)


def route_kernel(
    late, tokens, router, cotangent, sent, dispatch, combine, image, weights, pull, scratch, packed, sems
):
    width = image.shape[2]
    slots = weights.shape[1]
    tiles = 2 * width // LANES
    ways = sent.shape[1] // tiles
    loads = [
        pltpu.make_async_copy(src, dst, sems.at[k])
        for k, (src, dst) in enumerate(((tokens, image), (router, weights), (cotangent, pull)))
    ]
    for load in loads:
        load.start()
    loads[0].wait()
    loads[1].wait()
    logits = dot(image[0], weights[...], NN)
    up = jnp.exp(logits - jnp.max(logits, axis=0, keepdims=True))
    down = up / jnp.sum(up, axis=0, keepdims=True)
    dispatch[...] = down
    down = down.astype(jnp.bfloat16)
    up = jnp.exp(logits - jnp.max(logits, axis=1, keepdims=True))
    across = up / jnp.sum(up, axis=1, keepdims=True)
    combine[...] = across
    across = across.astype(jnp.bfloat16)
    for n in range(0, width, 256):
        spread(scratch, dot(down, image[0, :, n : n + 256], TN), 0, tiles, n)
    loads[2].wait()
    for n in range(0, width, 256):
        spread(scratch, dot(across, pull[0, :, n : n + 256], TN), tiles // 2, tiles, n)
    stores = []
    block = slots // BLOCKS
    for k in range(BLOCKS):
        part = pl.ds(k * block, block)
        piece = scratch[pl.ds(k * block * tiles, block * tiles), :].astype(jnp.bfloat16)
        piece = piece.reshape(block, tiles, LANES)
        for way in range(ways):
            packed[part, way * tiles : (way + 1) * tiles, :] = piece
        stores.append(pltpu.make_async_copy(packed.at[part], sent.at[part], sems.at[3 + k]))
        stores[-1].start()
    for store in stores:
        store.wait()
    pl.delay(late[0])


def route(late, tokens, router, cotangent, ways):
    _, count, width = tokens.shape
    slots = router.shape[1]
    tiles = 2 * width // LANES
    weights = jax.ShapeDtypeStruct((count, slots), jnp.float32)
    return pl.pallas_call(
        route_kernel,
        out_shape=(
            pltpu.HBM((slots, ways * tiles, LANES), jnp.bfloat16),
            weights,
            weights,
        ),
        in_specs=[pl.BlockSpec(memory_space=pltpu.SMEM)]
        + [pl.BlockSpec(memory_space=pltpu.HBM)] * 3,
        out_specs=(
            pl.BlockSpec(memory_space=pltpu.HBM),
            pl.BlockSpec(memory_space=pltpu.VMEM),
            pl.BlockSpec(memory_space=pltpu.VMEM),
        ),
        scratch_shapes=[
            pltpu.VMEM(tokens.shape, jnp.bfloat16),
            pltpu.VMEM(router.shape, jnp.bfloat16),
            pltpu.VMEM(tokens.shape, jnp.bfloat16),
            pltpu.VMEM((slots * tiles, LANES), jnp.float32),
            pltpu.VMEM((slots, ways * tiles, LANES), jnp.bfloat16),
            pltpu.SemaphoreType.DMA((3 + BLOCKS,)),
        ],
        compiler_params=pltpu.CompilerParams(vmem_limit_bytes=16 * 2**20),
        name="route",
    )(late, *in_hbm(tokens, router, cotangent))


def expert_kernel(
    arrived, in0, b0, out0, in1, b1, out1, sent, scratch, rows, grads, act, slope
):
    count, tiles, _ = arrived.shape
    half = tiles // 2
    width = half * LANES
    units = b0.shape[1]
    scratch[...] = arrived[...].astype(jnp.float32).reshape(count * tiles, LANES)
    gather(scratch, rows, count, 0, tiles)
    gather(scratch, grads, count, half, tiles)
    for h, (w_in, bias, w_out) in enumerate(
        ((in0.at[0], b0, out0.at[0]), (in1.at[0], b1, out1.at[0]))
    ):
        for u in range(0, units, UNITS):
            part = slice(u, u + UNITS)
            at = slice(h * units + u, h * units + u + UNITS)
            pre = dot(rows[...], w_in[:, part], NN) + bias[:, part]
            up = dot(grads[...], w_out[part, :], NT)
            square = pre * pre
            tanh = jnp.tanh(GELU_A * (pre + GELU_B * (square * pre)))
            cdf = 0.5 + 0.5 * tanh
            bend = 0.5 * GELU_A * pre * (1.0 - tanh * tanh) * (1.0 + 3.0 * GELU_B * square)
            act[:, at] = (pre * cdf).astype(jnp.bfloat16)
            slope[:, at] = (up * (cdf + bend)).astype(jnp.bfloat16)
    for n in range(0, width, 256):
        part = slice(n, n + 256)
        value = dot(act[:, :units], out0[0, :, part], NN) + dot(act[:, units:], out1[0, :, part], NN)
        spread(scratch, value, 0, tiles, n)
        value = dot(slope[:, :units], in0[0, part, :], NT) + dot(slope[:, units:], in1[0, part, :], NT)
        spread(scratch, value, half, tiles, n)
    sent[...] = scratch[...].astype(jnp.bfloat16).reshape(count, tiles, LANES)


def experts(arrived, own, other):
    count, tiles, _ = arrived.shape
    width = tiles // 2 * LANES
    units = own[1].shape[1]
    local = pl.BlockSpec(memory_space=pltpu.VMEM)
    return pl.pallas_call(
        expert_kernel,
        out_shape=jax.ShapeDtypeStruct(arrived.shape, jnp.bfloat16),
        in_specs=[local] * 7,
        out_specs=local,
        scratch_shapes=[
            pltpu.VMEM((count * tiles, LANES), jnp.float32),
            pltpu.VMEM((count, width), jnp.bfloat16),
            pltpu.VMEM((count, width), jnp.bfloat16),
            pltpu.VMEM((count, 2 * units), jnp.bfloat16),
            pltpu.VMEM((count, 2 * units), jnp.bfloat16),
        ],
        compiler_params=pltpu.CompilerParams(vmem_limit_bytes=28 * 2**20),
        name="experts",
    )(arrived, *own, *other)


def finish_kernel(
    returned,
    tokens,
    router,
    cotangent,
    dispatch,
    combine,
    mixed,
    token_grad,
    scratch,
    value,
    grad,
    near,
    far,
    sems,
):
    slots, width = value.shape
    tiles = 2 * width // LANES
    total = returned[:, :tiles, :].astype(jnp.float32)
    for way in range(1, returned.shape[1] // tiles):
        total = total + returned[:, way * tiles : (way + 1) * tiles, :].astype(jnp.float32)
    scratch[...] = total.reshape(slots * tiles, LANES)
    gather(scratch, value, slots, 0, tiles)
    gather(scratch, grad, slots, tiles // 2, tiles)
    down = dispatch[...]
    across = combine[...]
    near[0] = dot(across.astype(jnp.bfloat16), value[...], NN).astype(jnp.bfloat16)
    stores = [pltpu.make_async_copy(near, mixed, sems.at[0])]
    stores[0].start()
    pull = dot(cotangent[0], value[...], NT)
    slope = across * (pull - jnp.sum(across * pull, axis=1, keepdims=True))
    pull = dot(tokens[0], grad[...], NT)
    slope = slope + down * (pull - jnp.sum(down * pull, axis=0, keepdims=True))
    slope = slope.astype(jnp.bfloat16)
    down = down.astype(jnp.bfloat16)
    block = width // BLOCKS
    for k in range(BLOCKS):
        part = pl.ds(k * block, block)
        total = dot(down, grad[:, part], NN) + dot(slope, router[part, :], NT)
        far[0, :, part] = total.astype(jnp.bfloat16)
        stores.append(
            pltpu.make_async_copy(
                far.at[:, :, part], token_grad.at[:, :, part], sems.at[1 + k]
            )
        )
        stores[-1].start()
    for store in stores:
        store.wait()


def finish(returned, tokens, router, cotangent, dispatch, combine):
    width, slots = router.shape
    result = jax.ShapeDtypeStruct(tokens.shape, jnp.bfloat16)
    far = pl.BlockSpec(memory_space=pltpu.HBM)
    local = pl.BlockSpec(memory_space=pltpu.VMEM)
    return pl.pallas_call(
        finish_kernel,
        out_shape=(result, result),
        in_specs=[local] * 6,
        out_specs=(far, far),
        scratch_shapes=[
            pltpu.VMEM((slots * 2 * width // LANES, LANES), jnp.float32),
            pltpu.VMEM((slots, width), jnp.bfloat16),
            pltpu.VMEM((slots, width), jnp.bfloat16),
            pltpu.VMEM(tokens.shape, jnp.bfloat16),
            pltpu.VMEM(tokens.shape, jnp.bfloat16),
            pltpu.SemaphoreType.DMA((1 + BLOCKS,)),
        ],
        compiler_params=pltpu.CompilerParams(vmem_limit_bytes=16 * 2**20),
        name="finish",
    )(returned, tokens, router, cotangent, dispatch, combine)


def swap_cores(x):
    return lax.ppermute(x, "core", [(0, 1), (1, 0)])


def exchange(x):
    return lax.all_to_all(x, CHIPS, 0, 0, tiled=True)


def shards(tokens, router, w_in, b_in, w_out, cotangent):
    slots = router.shape[1]
    ways = lax.axis_size("yh")
    own = (w_in, b_in, w_out)
    other = tuple(swap_cores(w) for w in own)
    late = (lax.axis_index("core") * STAGGER_NS).reshape(1)
    sent, dispatch, combine = route(late, tokens, router, cotangent, ways)
    sent, *other = lax.optimization_barrier((sent, *other))
    tiles = sent.shape[1] // ways
    arrived = exchange(sent.reshape(slots * ways, tiles, LANES))
    returned = exchange(experts(arrived, own, other))
    returned = returned.reshape(slots, ways * tiles, LANES)
    return finish(returned, tokens, router, cotangent, dispatch, combine)


def solution(mesh):
    ways = mesh.shape["hidden"] // 2
    split = Mesh(
        mesh.devices.reshape(mesh.shape["expert"], ways, 2), ("expert", "yh", "core")
    )
    images = P(("expert", "yh", "core"), None, None)
    hidden = ("yh", "core")
    return jax.shard_map(
        shards,
        mesh=split,
        in_specs=(
            images,
            P(),
            P("expert", None, hidden),
            P("expert", hidden),
            P("expert", hidden, None),
            images,
        ),
        out_specs=(images, images),
        check_vma=False,
    )
```

```python
import jax
import jax.numpy as jnp
from jax import lax
from jax.experimental import pallas as pl
from jax.experimental.pallas import tpu as pltpu
from jax.sharding import Mesh, PartitionSpec as P

CHIPS = ("expert", "yh")
LANES = 128
UNITS = 256
BLOCKS = 4
PIECES = 1
STAGGER_NS = 8000
NN = (((1,), (0,)), ((), ()))
NT = (((1,), (1,)), ((), ()))
TN = (((0,), (0,)), ((), ()))
GELU_A = 0.7978845608028654
GELU_B = 0.044715


def in_hbm(*arrays):
    return [pltpu.with_memory_space_constraint(x, pltpu.HBM) for x in arrays]


def dot(a, b, dims):
    return lax.dot_general(a, b, dims, preferred_element_type=jnp.float32)


def spread(scratch, values, first, step, column):
    rows = values.shape[0]
    for k in range(values.shape[1] // LANES):
        piece = values[:, k * LANES : (k + 1) * LANES]
        scratch[pl.ds(first + column // LANES + k, rows, stride=step), :] = piece


def gather(scratch, out, rows, first, step):
    for k in range(out.shape[1] // LANES):
        piece = scratch[pl.ds(first + k, rows, stride=step), :]
        out[:, k * LANES : (k + 1) * LANES] = piece.astype(out.dtype)


def route_kernel(
    late, tokens, router, cotangent, sent, dispatch, combine, image, weights, pull, scratch, packed, sems
):
    width = image.shape[2]
    slots = weights.shape[1]
    tiles = 2 * width // LANES
    ways = sent.shape[1] // tiles
    loads = [
        pltpu.make_async_copy(src, dst, sems.at[k])
        for k, (src, dst) in enumerate(((tokens, image), (router, weights), (cotangent, pull)))
    ]
    for load in loads:
        load.start()
    loads[0].wait()
    loads[1].wait()
    logits = dot(image[0], weights[...], NN)
    up = jnp.exp(logits - jnp.max(logits, axis=0, keepdims=True))
    down = up / jnp.sum(up, axis=0, keepdims=True)
    dispatch[...] = down
    down = down.astype(jnp.bfloat16)
    up = jnp.exp(logits - jnp.max(logits, axis=1, keepdims=True))
    across = up / jnp.sum(up, axis=1, keepdims=True)
    combine[...] = across
    across = across.astype(jnp.bfloat16)
    for n in range(0, width, 256):
        spread(scratch, dot(down, image[0, :, n : n + 256], TN), 0, tiles, n)
    loads[2].wait()
    for n in range(0, width, 256):
        spread(scratch, dot(across, pull[0, :, n : n + 256], TN), tiles // 2, tiles, n)
    stores = []
    block = slots // BLOCKS
    for k in range(BLOCKS):
        part = pl.ds(k * block, block)
        piece = scratch[pl.ds(k * block * tiles, block * tiles), :].astype(jnp.bfloat16)
        piece = piece.reshape(block, tiles, LANES)
        for way in range(ways):
            packed[part, way * tiles : (way + 1) * tiles, :] = piece
        stores.append(pltpu.make_async_copy(packed.at[part], sent.at[part], sems.at[3 + k]))
        stores[-1].start()
    for store in stores:
        store.wait()
    pl.delay(late[0])


def route(late, tokens, router, cotangent, ways):
    _, count, width = tokens.shape
    slots = router.shape[1]
    tiles = 2 * width // LANES
    weights = jax.ShapeDtypeStruct((count, slots), jnp.float32)
    return pl.pallas_call(
        route_kernel,
        out_shape=(
            pltpu.HBM((slots, ways * tiles, LANES), jnp.bfloat16),
            weights,
            weights,
        ),
        in_specs=[pl.BlockSpec(memory_space=pltpu.SMEM)]
        + [pl.BlockSpec(memory_space=pltpu.HBM)] * 3,
        out_specs=(
            pl.BlockSpec(memory_space=pltpu.HBM),
            pl.BlockSpec(memory_space=pltpu.VMEM),
            pl.BlockSpec(memory_space=pltpu.VMEM),
        ),
        scratch_shapes=[
            pltpu.VMEM(tokens.shape, jnp.bfloat16),
            pltpu.VMEM(router.shape, jnp.bfloat16),
            pltpu.VMEM(tokens.shape, jnp.bfloat16),
            pltpu.VMEM((slots * tiles, LANES), jnp.float32),
            pltpu.VMEM((slots, ways * tiles, LANES), jnp.bfloat16),
            pltpu.SemaphoreType.DMA((3 + BLOCKS,)),
        ],
        compiler_params=pltpu.CompilerParams(vmem_limit_bytes=16 * 2**20),
        name="route",
    )(late, *in_hbm(tokens, router, cotangent))


def expert_kernel(
    arrived, in0, b0, out0, in1, b1, out1, sent, near, first, far, scratch, rows, grads, act, slope, sems
):
    count, tiles, _ = arrived.shape
    half = tiles // 2
    width = half * LANES
    units = b0.shape[1]
    loads = []
    for k, (src, dst) in enumerate(((out0, near), (in1, first), (out1, far))):
        block = dst.shape[0] // PIECES
        loads.append([])
        for p in range(PIECES):
            part = pl.ds(p * block, block)
            copy = pltpu.make_async_copy(src.at[0, part], dst.at[part], sems.at[k, p])
            loads[k].append(copy)
            copy.start()
    scratch[...] = arrived[...].astype(jnp.float32).reshape(count * tiles, LANES)
    gather(scratch, rows, count, 0, tiles)
    gather(scratch, grads, count, half, tiles)
    for h, (w_in, bias, w_out) in enumerate(((in0.at[0], b0, near), (first, b1, far))):
        if h:
            for load in loads[1]:
                load.wait()
        for u in range(0, units, UNITS):
            part = slice(u, u + UNITS)
            at = slice(h * units + u, h * units + u + UNITS)
            pre = dot(rows[...], w_in[:, part], NN) + bias[:, part]
            if u == 0:
                for load in loads[2 * h]:
                    load.wait()
            up = dot(grads[...], w_out[part, :], NT)
            square = pre * pre
            tanh = jnp.tanh(GELU_A * (pre + GELU_B * (square * pre)))
            cdf = 0.5 + 0.5 * tanh
            bend = 0.5 * GELU_A * pre * (1.0 - tanh * tanh) * (1.0 + 3.0 * GELU_B * square)
            act[:, at] = (pre * cdf).astype(jnp.bfloat16)
            slope[:, at] = (up * (cdf + bend)).astype(jnp.bfloat16)
    for n in range(0, width, 256):
        part = slice(n, n + 256)
        value = dot(act[:, :units], near[:, part], NN) + dot(act[:, units:], far[:, part], NN)
        spread(scratch, value, 0, tiles, n)
        value = dot(slope[:, :units], in0[0, part, :], NT) + dot(slope[:, units:], first[part, :], NT)
        spread(scratch, value, half, tiles, n)
    sent[...] = scratch[...].astype(jnp.bfloat16).reshape(count, tiles, LANES)


def experts(arrived, own, other):
    count, tiles, _ = arrived.shape
    width = tiles // 2 * LANES
    units = own[1].shape[1]
    out0, in1, out1 = in_hbm(own[2], other[0], other[2])
    weight = pl.BlockSpec(memory_space=pltpu.HBM)
    local = pl.BlockSpec(memory_space=pltpu.VMEM)
    return pl.pallas_call(
        expert_kernel,
        out_shape=jax.ShapeDtypeStruct(arrived.shape, jnp.bfloat16),
        in_specs=[local, local, local, weight, weight, local, weight],
        out_specs=local,
        scratch_shapes=[
            pltpu.VMEM((units, width), jnp.bfloat16),
            pltpu.VMEM((width, units), jnp.bfloat16),
            pltpu.VMEM((units, width), jnp.bfloat16),
            pltpu.VMEM((count * tiles, LANES), jnp.float32),
            pltpu.VMEM((count, width), jnp.bfloat16),
            pltpu.VMEM((count, width), jnp.bfloat16),
            pltpu.VMEM((count, 2 * units), jnp.bfloat16),
            pltpu.VMEM((count, 2 * units), jnp.bfloat16),
            pltpu.SemaphoreType.DMA((3, PIECES)),
        ],
        compiler_params=pltpu.CompilerParams(vmem_limit_bytes=28 * 2**20),
        name="experts",
    )(arrived, own[0], own[1], out0, in1, other[1], out1)


def finish_kernel(
    returned,
    tokens,
    router,
    cotangent,
    dispatch,
    combine,
    mixed,
    token_grad,
    scratch,
    value,
    grad,
    near,
    far,
    sems,
):
    slots, width = value.shape
    tiles = 2 * width // LANES
    total = returned[:, :tiles, :].astype(jnp.float32)
    for way in range(1, returned.shape[1] // tiles):
        total = total + returned[:, way * tiles : (way + 1) * tiles, :].astype(jnp.float32)
    scratch[...] = total.reshape(slots * tiles, LANES)
    gather(scratch, value, slots, 0, tiles)
    gather(scratch, grad, slots, tiles // 2, tiles)
    down = dispatch[...]
    across = combine[...]
    near[0] = dot(across.astype(jnp.bfloat16), value[...], NN).astype(jnp.bfloat16)
    stores = [pltpu.make_async_copy(near, mixed, sems.at[0])]
    stores[0].start()
    pull = dot(cotangent[0], value[...], NT)
    slope = across * (pull - jnp.sum(across * pull, axis=1, keepdims=True))
    pull = dot(tokens[0], grad[...], NT)
    slope = slope + down * (pull - jnp.sum(down * pull, axis=0, keepdims=True))
    slope = slope.astype(jnp.bfloat16)
    down = down.astype(jnp.bfloat16)
    block = width // BLOCKS
    for k in range(BLOCKS):
        part = pl.ds(k * block, block)
        total = dot(down, grad[:, part], NN) + dot(slope, router[part, :], NT)
        far[0, :, part] = total.astype(jnp.bfloat16)
        stores.append(
            pltpu.make_async_copy(
                far.at[:, :, part], token_grad.at[:, :, part], sems.at[1 + k]
            )
        )
        stores[-1].start()
    for store in stores:
        store.wait()


def finish(returned, tokens, router, cotangent, dispatch, combine):
    width, slots = router.shape
    result = jax.ShapeDtypeStruct(tokens.shape, jnp.bfloat16)
    far = pl.BlockSpec(memory_space=pltpu.HBM)
    local = pl.BlockSpec(memory_space=pltpu.VMEM)
    return pl.pallas_call(
        finish_kernel,
        out_shape=(result, result),
        in_specs=[local] * 6,
        out_specs=(far, far),
        scratch_shapes=[
            pltpu.VMEM((slots * 2 * width // LANES, LANES), jnp.float32),
            pltpu.VMEM((slots, width), jnp.bfloat16),
            pltpu.VMEM((slots, width), jnp.bfloat16),
            pltpu.VMEM(tokens.shape, jnp.bfloat16),
            pltpu.VMEM(tokens.shape, jnp.bfloat16),
            pltpu.SemaphoreType.DMA((1 + BLOCKS,)),
        ],
        compiler_params=pltpu.CompilerParams(vmem_limit_bytes=16 * 2**20),
        name="finish",
    )(returned, tokens, router, cotangent, dispatch, combine)


def swap_cores(x):
    return lax.ppermute(x, "core", [(0, 1), (1, 0)])


def exchange(x):
    return lax.all_to_all(x, CHIPS, 0, 0, tiled=True)


def shards(tokens, router, w_in, b_in, w_out, cotangent):
    slots = router.shape[1]
    ways = lax.axis_size("yh")
    own = (w_in, b_in, w_out)
    other = tuple(swap_cores(w) for w in own)
    late = (lax.axis_index("core") * STAGGER_NS).reshape(1)
    sent, dispatch, combine = route(late, tokens, router, cotangent, ways)
    tiles = sent.shape[1] // ways
    arrived = exchange(sent.reshape(slots * ways, tiles, LANES))
    returned = exchange(experts(arrived, own, other))
    returned = returned.reshape(slots, ways * tiles, LANES)
    return finish(returned, tokens, router, cotangent, dispatch, combine)


def solution(mesh):
    ways = mesh.shape["hidden"] // 2
    split = Mesh(
        mesh.devices.reshape(mesh.shape["expert"], ways, 2), ("expert", "yh", "core")
    )
    images = P(("expert", "yh", "core"), None, None)
    hidden = ("yh", "core")
    return jax.shard_map(
        shards,
        mesh=split,
        in_specs=(
            images,
            P(),
            P("expert", None, hidden),
            P("expert", hidden),
            P("expert", hidden, None),
            images,
        ),
        out_specs=(images, images),
        check_vma=False,
    )
```
